32 devices in a mesh: shard: 2 (over core), width: 4 (over y, x), shift: 4 (over z).
Axes of the slice: x: 2, y: 2, z: 4, core: 2. Of those that a mesh axis runs over, the one named last changes fastest.
Arguments:
- w_query: float32 [16384, 4096], P(('shift', 'shard'), 'width'), parts along dimension 0, may hold values from -0.125 to 0.125
- first_query: float32 [16384, 4096], P(('shift', 'shard'), 'width'), parts along dimension 0, may hold values from -0.09375 to 0.09375
- second_query: float32 [16384, 4096], P(('shift', 'shard'), 'width'), parts along dimension 0, may hold values from -0.09375 to 0.09375
- w_key: float32 [16384, 1024], P(('shift', 'shard'), 'width'), parts along dimension 0, may hold values from -0.125 to 0.125
- first_key: float32 [16384, 1024], P(('shift', 'shard'), 'width'), parts along dimension 0, may hold values from -0.09375 to 0.09375
- second_key: float32 [16384, 1024], P(('shift', 'shard'), 'width'), parts along dimension 0, may hold values from -0.09375 to 0.09375
- w_value: float32 [16384, 1024], P(('shift', 'shard'), 'width'), parts along dimension 0, may hold values from -0.125 to 0.125
- first_value: float32 [16384, 1024], P(('shift', 'shard'), 'width'), parts along dimension 0, may hold values from -0.09375 to 0.09375
- second_value: float32 [16384, 1024], P(('shift', 'shard'), 'width'), parts along dimension 0, may hold values from -0.09375 to 0.09375
- norm_gain: float32 [16384], P(('shift', 'shard')), parts along dimension 0, may hold values from 0.25 to 1.75
Outputs:
- ready_query: bfloat16 [16384, 4096], P('shift', 'width'), parts along dimension 0
- ready_key: bfloat16 [16384, 1024], P('shift', 'width'), parts along dimension 0
- ready_value: bfloat16 [16384, 1024], P('shift', 'width'), parts along dimension 0
- scale_query: float32 [16384], P(('shift', 'width')), parts along dimension 0
- scale_key: float32 [4096], P(('shift', 'width')), parts along dimension 0
- scale_value: float32 [4096], P(('shift', 'width')), parts along dimension 0
The draws below stay inside these ranges and needn't reach their ends.
There are 4 independent parts, one for each index of `shift`. The reference program is written for one: setup_inputs(seed, part) draws one part's arguments, and reference() takes and returns one part's arrays. A program takes and returns all parts, laid end to end along the dimension named above; each array names one. Nothing has to cross between parts.
All inputs are finite; a program needn't handle non-finite values. Where the reference program divides by a largest or mean magnitude, that divisor is 1e-20 or more.
Results may differ from the reference program's by a relative error of at most 0.001.
Values may be sent and summed in bfloat16 or wider, within the bound.
A program may use at most 128 MiB of HBM per device.

```python
import jax
import jax.numpy as jnp

D_MODEL = 4096
Q_DIM = 4096
KV_DIM = 1024


def spiked(drawn, own_key, source, target, blocks, factor):
    owner, partner = [(jnp.arange(drawn.shape[axis_at]) // (drawn.shape[axis_at] // blocks)).reshape([-1 if axis == axis_at else 1 for axis in range(drawn.ndim)]) for axis_at in (source, target)]
    chosen = jax.random.permutation(own_key, blocks)[partner]
    strong = (owner == chosen) | (owner == (partner + blocks // 2) % blocks)
    return jnp.where(strong, factor * drawn, drawn)


def levels(rng, extent, shards, least, high):
    loudness, own = 1.0, jax.random.fold_in(rng, 6)
    for dim, blocks in shards:
        heights = jnp.exp(jax.random.uniform(jax.random.fold_in(own, dim), (blocks,), jnp.float32, least / len(shards), high / len(shards)))
        loudness = loudness * jnp.repeat(heights, extent[dim] // blocks).reshape([-1 if axis == dim else 1 for axis in range(len(extent))])
    return loudness


def noise(own_key, dims, deviation, limit, split=(), kind=jnp.bfloat16):
    array = deviation * jax.random.normal(own_key, dims, jnp.float32)
    if split:
        array = array * levels(own_key, dims, split, -0.22, 0.18)
    return jnp.clip(array, -limit, limit).astype(kind)


def bell_draw_with(own_key, extent, spread, limit, cuts, heavy, held_as=jnp.bfloat16):
    array = spread * jax.random.normal(own_key, extent, jnp.float32)
    if cuts:
        array = array * levels(own_key, extent, cuts, -0.22, 0.18)
    return jnp.clip(spiked(array, jax.random.fold_in(own_key, 3), *heavy), -limit, limit).astype(held_as)


def setup_inputs(seed: int = 0, part: int = 0) -> dict:
    arg_keys = jax.random.split(jax.random.key(seed), 11)
    part_splits = jax.random.split(jax.random.fold_in(arg_keys[10], part), 11)
    w_query = bell_draw_with(part_splits[0], (D_MODEL, Q_DIM), D_MODEL ** -0.5, 0.125, ((0, 2), (1, 4)), (0, 1, 4, 2.0), jnp.float32)
    first_query = noise(part_splits[1], (D_MODEL, Q_DIM), D_MODEL ** -0.5, 0.09375, ((0, 2), (1, 4)), jnp.float32)
    second_query = noise(part_splits[2], (D_MODEL, Q_DIM), D_MODEL ** -0.5, 0.09375, ((0, 2), (1, 4)), jnp.float32)
    w_key = bell_draw_with(part_splits[3], (D_MODEL, KV_DIM), D_MODEL ** -0.5, 0.125, ((0, 2), (1, 4)), (0, 1, 4, 2.0), jnp.float32)
    first_key = noise(part_splits[4], (D_MODEL, KV_DIM), D_MODEL ** -0.5, 0.09375, ((0, 2), (1, 4)), jnp.float32)
    second_key = noise(part_splits[5], (D_MODEL, KV_DIM), D_MODEL ** -0.5, 0.09375, ((0, 2), (1, 4)), jnp.float32)
    w_value = bell_draw_with(part_splits[6], (D_MODEL, KV_DIM), D_MODEL ** -0.5, 0.125, ((0, 2), (1, 4)), (0, 1, 4, 2.0), jnp.float32)
    first_value = noise(part_splits[7], (D_MODEL, KV_DIM), D_MODEL ** -0.5, 0.09375, ((0, 2), (1, 4)), jnp.float32)
    second_value = noise(part_splits[8], (D_MODEL, KV_DIM), D_MODEL ** -0.5, 0.09375, ((0, 2), (1, 4)), jnp.float32)
    norm_gain = jnp.clip(1.0 + 0.15 * jax.random.normal(part_splits[9], (D_MODEL,), jnp.float32), 0.25, 1.75)
    return dict(w_query=w_query, first_query=first_query, second_query=second_query, w_key=w_key, first_key=first_key, second_key=second_key, w_value=w_value, first_value=first_value, second_value=second_value, norm_gain=norm_gain)


learn_rate = 0.25
hold_rate = 0.8


def reference(w_query, first_query, second_query, w_key, first_key, second_key, w_value, first_value, second_value, norm_gain):
    hold_query = hold_rate * first_query + second_query
    latest_query = w_query - learn_rate * hold_query
    hold_key = hold_rate * first_key + second_key
    latest_key = w_key - learn_rate * hold_key
    hold_value = hold_rate * first_value + second_value
    latest_value = w_value - learn_rate * hold_value
    latest_gained_query = latest_query * norm_gain[:, None]
    latest_gained_key = latest_key * norm_gain[:, None]
    latest_gained_value = latest_value * norm_gain[:, None]
    scale_query = jnp.max(jnp.abs(latest_gained_query), axis=0)
    ready_query = (latest_gained_query / scale_query).astype(jnp.bfloat16)
    scale_key = jnp.max(jnp.abs(latest_gained_key), axis=0)
    ready_key = (latest_gained_key / scale_key).astype(jnp.bfloat16)
    scale_value = jnp.max(jnp.abs(latest_gained_value), axis=0)
    ready_value = (latest_gained_value / scale_value).astype(jnp.bfloat16)
    return ready_query, ready_key, ready_value, scale_query, scale_key, scale_value
```

```python
import functools

import jax
import jax.numpy as jnp
from jax import lax
from jax.experimental import pallas as pl
from jax.experimental.pallas import tpu as pltpu
from jax.sharding import PartitionSpec as P

learn_rate = 0.25
hold_rate = 0.8

LANES = 128
SUBLANES = 8
STEP_ROWS = 128
AHEAD = 6
MESH = pl.DeviceIdType.MESH


def exchange_kernel(peers, chunks, *refs):
    gain_ref, sources, readies, scales = refs[0], refs[1:10], refs[10:13], refs[13:16]
    held, gains, peaks, arrived, in_sem, peak_send, peak_recv, out_send, out_recv = refs[16:]
    rows = gains.shape[0]
    me = lax.axis_index("shard")
    others = [lax.rem(me + k, peers) for k in range(1, peers)]
    my_rows = pl.ds(pl.multiple_of(me * rows, rows), rows)

    def reads(c):
        which, col = chunks[c]
        return [
            pltpu.make_async_copy(
                sources[3 * which + i].at[:, pl.ds(col * LANES, LANES)],
                held.at[i, c],
                in_sem.at[i, c],
            )
            for i in range(3)
        ]

    for c in range(min(AHEAD, len(chunks))):
        for read in reads(c):
            read.start()

    barrier = pltpu.get_barrier_semaphore()
    for other in others:
        pl.semaphore_signal(barrier, inc=1, device_id={"shard": other}, device_id_type=MESH)

    for j in range(rows // LANES):
        spread = jnp.broadcast_to(gain_ref[pl.ds(j, 1), :], (LANES, LANES))
        gains[pl.ds(j * LANES, LANES), :] = spread.T

    pl.semaphore_wait(barrier, peers - 1)

    def update(c):
        def step(r, peak):
            here = pl.ds(pl.multiple_of(r * STEP_ROWS, STEP_ROWS), STEP_ROWS)
            hold = hold_rate * held[1, c, here, :] + held[2, c, here, :]
            gained = (held[0, c, here, :] - learn_rate * hold) * gains[here, :]
            held[0, c, here, :] = gained
            tiles = jnp.abs(gained).reshape(STEP_ROWS // SUBLANES, SUBLANES, LANES)
            return jnp.maximum(peak, jnp.max(tiles, axis=0))

        peaks[c] = lax.fori_loop(
            0, rows // STEP_ROWS, step, jnp.zeros((SUBLANES, LANES), jnp.float32)
        )

    def peak_copy(c, k):
        return pltpu.make_async_remote_copy(
            src_ref=peaks.at[c],
            dst_ref=arrived.at[k, c],
            send_sem=peak_send.at[k, c],
            recv_sem=peak_recv.at[k, c],
            device_id={"shard": others[k]},
            device_id_type=MESH,
        )

    def scale_and_round(c):
        which, col = chunks[c]
        peak = peaks[c]
        for k in range(peers - 1):
            peak_copy(c, k).wait_recv()
            peak = jnp.maximum(peak, arrived[k, c])
        scale = jnp.max(peak, axis=0, keepdims=True)
        scales[which][pl.ds(col, 1), :] = scale
        inverse = jnp.broadcast_to(1.0 / scale, (STEP_ROWS, LANES))
        columns = pl.ds(col * LANES, LANES)

        def step(r, _):
            here = pl.ds(pl.multiple_of(r * STEP_ROWS, STEP_ROWS), STEP_ROWS)
            there = pl.ds(pl.multiple_of(me * rows + r * STEP_ROWS, STEP_ROWS), STEP_ROWS)
            readies[which][there, columns] = (held[0, c, here, :] * inverse).astype(jnp.bfloat16)
            return 0

        lax.fori_loop(0, rows // STEP_ROWS, step, 0)

    def out_copy(c, k):
        which, col = chunks[c]
        block = readies[which].at[my_rows, pl.ds(col * LANES, LANES)]
        return pltpu.make_async_remote_copy(
            src_ref=block,
            dst_ref=block,
            send_sem=out_send.at[k, c],
            recv_sem=out_recv.at[k, c],
            device_id={"shard": others[k]},
            device_id_type=MESH,
        )

    for c in range(len(chunks) + 1):
        if c < len(chunks):
            for read in reads(c):
                read.wait()
            if c + AHEAD < len(chunks):
                for read in reads(c + AHEAD):
                    read.start()
            update(c)
            for k in range(peers - 1):
                peak_copy(c, k).start()
        if c >= 1:
            scale_and_round(c - 1)
            for k in range(peers - 1):
                out_copy(c - 1, k).start()

    for c in range(len(chunks)):
        for k in range(peers - 1):
            peak_copy(c, k).wait_send()
            out_copy(c, k).wait_send()
            out_copy(c, k).wait_recv()


def store_kernel(pieces, *refs):
    half = len(refs) // 2
    sources, targets, sem = refs[:half], refs[half : 2 * half], refs[-1]
    copies = []
    for source, target in zip(sources, targets):
        parts = pieces if source.shape[0] % (pieces * LANES) == 0 else 1
        size = source.shape[0] // parts
        for p in range(parts):
            where = pl.ds(p * size, size)
            copies.append(
                pltpu.make_async_copy(source.at[where], target.at[where], sem.at[len(copies)])
            )
    for copy in copies:
        copy.start()
    for copy in copies:
        copy.wait()


def body(*arrays):
    *weights, norm_gain = arrays
    peers = lax.axis_size("shard")
    rows = norm_gain.shape[0]
    widths = [weights[3 * which].shape[1] for which in range(3)]
    chunks = [(which, col) for which in range(3) for col in range(widths[which] // LANES)]
    count = len(chunks)
    any_spec = pl.BlockSpec(memory_space=pltpu.HBM)
    vmem_spec = pl.BlockSpec(memory_space=pltpu.VMEM)
    ready_shapes = [((peers * rows, width), jnp.bfloat16) for width in widths]
    scale_shapes = [((width // LANES, LANES), jnp.float32) for width in widths]
    made = pl.pallas_call(
        functools.partial(exchange_kernel, peers, chunks),
        out_shape=[pltpu.VMEM(*s) for s in ready_shapes + scale_shapes],
        in_specs=[vmem_spec] + [any_spec] * 9,
        out_specs=[vmem_spec] * 6,
        scratch_shapes=[
            pltpu.VMEM((3, count, rows, LANES), jnp.float32),
            pltpu.VMEM((rows, LANES), jnp.float32),
            pltpu.VMEM((count, SUBLANES, LANES), jnp.float32),
            pltpu.VMEM((peers - 1, count, SUBLANES, LANES), jnp.float32),
            pltpu.SemaphoreType.DMA((3, count)),
            pltpu.SemaphoreType.DMA((peers - 1, count)),
            pltpu.SemaphoreType.DMA((peers - 1, count)),
            pltpu.SemaphoreType.DMA((peers - 1, count)),
            pltpu.SemaphoreType.DMA((peers - 1, count)),
        ],
        compiler_params=pltpu.CompilerParams(
            collective_id=0, has_side_effects=True, vmem_limit_bytes=44 * 1024 * 1024
        ),
        name="exchange",
    )(norm_gain.reshape(rows // LANES, LANES), *weights)
    pieces = 4
    stored = pl.pallas_call(
        functools.partial(store_kernel, pieces),
        out_shape=[jax.ShapeDtypeStruct(*s) for s in ready_shapes + scale_shapes],
        in_specs=[vmem_spec] * 6,
        out_specs=[any_spec] * 6,
        scratch_shapes=[pltpu.SemaphoreType.DMA((6 * pieces,))],
        compiler_params=pltpu.CompilerParams(vmem_limit_bytes=2 * 1024 * 1024),
        name="store",
    )(*made)
    return (*stored[:3], *(s.reshape(-1) for s in stored[3:]))


def solution(mesh):
    split = P(("shift", "shard"), "width")
    in_specs = (split,) * 9 + (P(("shift", "shard")),)
    out_specs = (P("shift", "width"),) * 3 + (P(("shift", "width")),) * 3
    return jax.shard_map(body, mesh=mesh, in_specs=in_specs, out_specs=out_specs, check_vma=False)
```

```python
import functools

import jax
import jax.numpy as jnp
from jax import lax
from jax.experimental import pallas as pl
from jax.experimental.pallas import tpu as pltpu
from jax.sharding import PartitionSpec as P

learn_rate = 0.25
hold_rate = 0.8

LANES = 128
SUBLANES = 8
STEP_ROWS = 64
AHEAD = 12
PIECES = 4
MESH = pl.DeviceIdType.MESH


def exchange_kernel(peers, chunks, *refs):
    gain_ref, sources, readies, scales = refs[0], refs[1:10], refs[10:13], refs[13:16]
    gain_held, held, gains, peaks, arrived, gain_sem, in_sem, peak_send, peak_recv, out_send, out_recv = refs[16:]
    rows = gains.shape[0]
    me = lax.axis_index("shard")
    others = [lax.rem(me + k, peers) for k in range(1, peers)]
    my_rows = pl.ds(pl.multiple_of(me * rows, rows), rows)

    last = len(chunks) - 1
    piece_rows = rows // PIECES

    def reads(c, piece=None):
        which, col = chunks[c]
        some = pl.ds(0, rows) if piece is None else pl.ds(piece * piece_rows, piece_rows)
        return [
            pltpu.make_async_copy(
                sources[3 * which + i].at[some, pl.ds(col * LANES, LANES)],
                held.at[i, c, some],
                in_sem.at[i, c + (piece or 0)],
            )
            for i in range(3)
        ]

    def start_reads(c):
        for piece in range(PIECES) if c == last else (None,):
            for read in reads(c, piece):
                read.start()

    gain_read = pltpu.make_async_copy(gain_ref, gain_held, gain_sem)
    gain_read.start()

    for c in range(min(1, len(chunks))):
        start_reads(c)

    barrier = pltpu.get_barrier_semaphore()
    for other in others:
        pl.semaphore_signal(barrier, inc=1, device_id={"shard": other}, device_id_type=MESH)

    gain_read.wait()
    for c in range(min(1, len(chunks)), min(AHEAD, len(chunks))):
        start_reads(c)
    for j in range(rows // LANES):
        spread = jnp.broadcast_to(gain_held[pl.ds(j, 1), :], (LANES, LANES))
        gains[pl.ds(j * LANES, LANES), :] = spread.T

    pl.semaphore_wait(barrier, peers - 1)

    def update(c, first, count, peak):
        def step(r, peak):
            here = pl.ds(pl.multiple_of(r * STEP_ROWS, STEP_ROWS), STEP_ROWS)
            hold = hold_rate * held[1, c, here, :] + held[2, c, here, :]
            gained = (held[0, c, here, :] - learn_rate * hold) * gains[here, :]
            held[0, c, here, :] = gained
            tiles = jnp.abs(gained).reshape(STEP_ROWS // SUBLANES, SUBLANES, LANES)
            return jnp.maximum(peak, jnp.max(tiles, axis=0))

        return lax.fori_loop(first // STEP_ROWS, (first + count) // STEP_ROWS, step, peak)

    def peak_copy(c, k):
        return pltpu.make_async_remote_copy(
            src_ref=peaks.at[c],
            dst_ref=arrived.at[k, c],
            send_sem=peak_send.at[k, c],
            recv_sem=peak_recv.at[k, c],
            device_id={"shard": others[k]},
            device_id_type=MESH,
        )

    def scale_and_round(c):
        which, col = chunks[c]
        peak = peaks[c]
        for k in range(peers - 1):
            peak_copy(c, k).wait_recv()
            peak = jnp.maximum(peak, arrived[k, c])
        scale = jnp.max(peak, axis=0, keepdims=True)
        scales[which][pl.ds(col, 1), :] = scale
        inverse = jnp.broadcast_to(1.0 / scale, (STEP_ROWS, LANES))
        columns = pl.ds(col * LANES, LANES)

        def step(r, _):
            here = pl.ds(pl.multiple_of(r * STEP_ROWS, STEP_ROWS), STEP_ROWS)
            there = pl.ds(pl.multiple_of(me * rows + r * STEP_ROWS, STEP_ROWS), STEP_ROWS)
            readies[which][there, columns] = (held[0, c, here, :] * inverse).astype(jnp.bfloat16)
            return 0

        for piece in range(PIECES):
            first = piece * piece_rows
            lax.fori_loop(first // STEP_ROWS, (first + piece_rows) // STEP_ROWS, step, 0)
            for k in range(peers - 1):
                out_copy(c, k, piece).start()

    def out_copy(c, k, piece=None):
        which, col = chunks[c]
        some = my_rows
        if piece is not None:
            some = pl.ds(pl.multiple_of(me * rows + piece * piece_rows, piece_rows), piece_rows)
        block = readies[which].at[some, pl.ds(col * LANES, LANES)]
        return pltpu.make_async_remote_copy(
            src_ref=block,
            dst_ref=block,
            send_sem=out_send.at[k, c],
            recv_sem=out_recv.at[k, c],
            device_id={"shard": others[k]},
            device_id_type=MESH,
        )

    for c in range(len(chunks) + 1):
        if c < len(chunks):
            peak = jnp.zeros((SUBLANES, LANES), jnp.float32)
            if c == last:
                for piece in range(PIECES):
                    for read in reads(c, piece):
                        read.wait()
                    peak = update(c, piece * piece_rows, piece_rows, peak)
            else:
                for read in reads(c):
                    read.wait()
                if c + AHEAD <= last:
                    start_reads(c + AHEAD)
                peak = update(c, 0, rows, peak)
            peaks[c] = peak
            for k in range(peers - 1):
                peak_copy(c, k).start()
        if c >= 1:
            scale_and_round(c - 1)

    for c in range(len(chunks)):
        for k in range(peers - 1):
            peak_copy(c, k).wait_send()
            out_copy(c, k).wait_send()
            out_copy(c, k).wait_recv()


def store_kernel(pieces, *refs):
    half = len(refs) // 2
    sources, targets, sem = refs[:half], refs[half : 2 * half], refs[-1]
    copies = []
    for source, target in zip(sources, targets):
        parts = pieces if source.shape[0] % (pieces * LANES) == 0 else 1
        size = source.shape[0] // parts
        for p in range(parts):
            where = pl.ds(p * size, size)
            copies.append(
                pltpu.make_async_copy(source.at[where], target.at[where], sem.at[len(copies)])
            )
    for copy in copies:
        copy.start()
    for copy in copies:
        copy.wait()


def body(*arrays):
    *weights, norm_gain = arrays
    peers = lax.axis_size("shard")
    rows = norm_gain.shape[0]
    widths = [weights[3 * which].shape[1] for which in range(3)]
    chunks = [(which, col) for which in range(3) for col in range(widths[which] // LANES)]
    count = len(chunks)
    any_spec = pl.BlockSpec(memory_space=pltpu.HBM)
    vmem_spec = pl.BlockSpec(memory_space=pltpu.VMEM)
    ready_shapes = [((peers * rows, width), jnp.bfloat16) for width in widths]
    scale_shapes = [((width // LANES, LANES), jnp.float32) for width in widths]
    made = pl.pallas_call(
        functools.partial(exchange_kernel, peers, chunks),
        out_shape=[pltpu.VMEM(*s) for s in ready_shapes + scale_shapes],
        in_specs=[any_spec] * 10,
        out_specs=[vmem_spec] * 6,
        scratch_shapes=[
            pltpu.VMEM((rows // LANES, LANES), jnp.float32),
            pltpu.VMEM((3, count, rows, LANES), jnp.float32),
            pltpu.VMEM((rows, LANES), jnp.float32),
            pltpu.VMEM((count, SUBLANES, LANES), jnp.float32),
            pltpu.VMEM((peers - 1, count, SUBLANES, LANES), jnp.float32),
            pltpu.SemaphoreType.DMA,
            pltpu.SemaphoreType.DMA((3, count + PIECES - 1)),
            pltpu.SemaphoreType.DMA((peers - 1, count)),
            pltpu.SemaphoreType.DMA((peers - 1, count)),
            pltpu.SemaphoreType.DMA((peers - 1, count)),
            pltpu.SemaphoreType.DMA((peers - 1, count)),
        ],
        compiler_params=pltpu.CompilerParams(
            collective_id=0, has_side_effects=True, vmem_limit_bytes=44 * 1024 * 1024
        ),
        name="exchange",
    )(norm_gain.reshape(rows // LANES, LANES), *weights)
    pieces = 2
    stored = pl.pallas_call(
        functools.partial(store_kernel, pieces),
        out_shape=[jax.ShapeDtypeStruct(*s) for s in ready_shapes + scale_shapes],
        in_specs=[vmem_spec] * 6,
        out_specs=[any_spec] * 6,
        scratch_shapes=[pltpu.SemaphoreType.DMA((6 * pieces,))],
        compiler_params=pltpu.CompilerParams(vmem_limit_bytes=2 * 1024 * 1024),
        name="store",
    )(*made)
    return (*stored[:3], *(s.reshape(-1) for s in stored[3:]))


def solution(mesh):
    split = P(("shift", "shard"), "width")
    in_specs = (split,) * 9 + (P(("shift", "shard")),)
    out_specs = (P("shift", "width"),) * 3 + (P(("shift", "width")),) * 3
    return jax.shard_map(body, mesh=mesh, in_specs=in_specs, out_specs=out_specs, check_vma=False)
```

```python
import functools

import jax
import jax.numpy as jnp
from jax import lax
from jax.experimental import pallas as pl
from jax.experimental.pallas import tpu as pltpu
from jax.sharding import PartitionSpec as P

learn_rate = 0.25
hold_rate = 0.8

LANES = 128
SUBLANES = 8
STEP_ROWS = 128
AHEAD = 12
PIECES = 4
MESH = pl.DeviceIdType.MESH


def exchange_kernel(peers, chunks, *refs):
    gain_ref, sources, readies, scales = refs[0], refs[1:10], refs[10:13], refs[13:16]
    gain_held, held, gains, peaks, arrived, gain_sem, in_sem, peak_send, peak_recv, out_send, out_recv = refs[16:]
    rows = gains.shape[0]
    me = lax.axis_index("shard")
    others = [lax.rem(me + k, peers) for k in range(1, peers)]
    my_rows = pl.ds(pl.multiple_of(me * rows, rows), rows)

    last = len(chunks) - 1
    piece_rows = rows // PIECES
    step_rows = min(STEP_ROWS, piece_rows)

    def reads(c, piece=None):
        which, col = chunks[c]
        some = pl.ds(0, rows) if piece is None else pl.ds(piece * piece_rows, piece_rows)
        return [
            pltpu.make_async_copy(
                sources[3 * which + i].at[some, pl.ds(col * LANES, LANES)],
                held.at[i, c, some],
                in_sem.at[i, c + (piece or 0)],
            )
            for i in range(3)
        ]

    def start_reads(c):
        for piece in range(PIECES) if c == last else (None,):
            for read in reads(c, piece):
                read.start()

    gain_read = pltpu.make_async_copy(gain_ref, gain_held, gain_sem)
    gain_read.start()

    barrier = pltpu.get_barrier_semaphore()
    for other in others:
        pl.semaphore_signal(barrier, inc=1, device_id={"shard": other}, device_id_type=MESH)

    pl.semaphore_wait(barrier, peers - 1)
    for c in range(min(AHEAD, len(chunks))):
        start_reads(c)

    gain_read.wait()
    for j in range(rows // LANES):
        spread = jnp.broadcast_to(gain_held[pl.ds(j, 1), :], (LANES, LANES))
        gains[pl.ds(j * LANES, LANES), :] = spread.T


    def update(c, first, count, peak):
        def step(r, peak):
            here = pl.ds(pl.multiple_of(r * step_rows, step_rows), step_rows)
            hold = hold_rate * held[1, c, here, :] + held[2, c, here, :]
            gained = (held[0, c, here, :] - learn_rate * hold) * gains[here, :]
            held[0, c, here, :] = gained
            tiles = jnp.abs(gained).reshape(step_rows // SUBLANES, SUBLANES, LANES)
            return jnp.maximum(peak, jnp.max(tiles, axis=0))

        return lax.fori_loop(first // step_rows, (first + count) // step_rows, step, peak)

    def peak_copy(c, k):
        return pltpu.make_async_remote_copy(
            src_ref=peaks.at[c],
            dst_ref=arrived.at[k, c],
            send_sem=peak_send.at[k, c],
            recv_sem=peak_recv.at[k, c],
            device_id={"shard": others[k]},
            device_id_type=MESH,
        )

    def scale_and_round(c):
        which, col = chunks[c]
        peak = peaks[c]
        for k in range(peers - 1):
            peak_copy(c, k).wait_recv()
            peak = jnp.maximum(peak, arrived[k, c])
        scale = jnp.max(peak, axis=0, keepdims=True)
        scales[which][pl.ds(col, 1), :] = scale
        inverse = jnp.broadcast_to(1.0 / scale, (step_rows, LANES))
        columns = pl.ds(col * LANES, LANES)

        def step(r, _):
            here = pl.ds(pl.multiple_of(r * step_rows, step_rows), step_rows)
            there = pl.ds(pl.multiple_of(me * rows + r * step_rows, step_rows), step_rows)
            readies[which][there, columns] = (held[0, c, here, :] * inverse).astype(jnp.bfloat16)
            return 0

        for piece in range(PIECES):
            first = piece * piece_rows
            lax.fori_loop(first // step_rows, (first + piece_rows) // step_rows, step, 0)
            for k in range(peers - 1):
                out_copy(c, k, piece).start()

    def out_copy(c, k, piece=None):
        which, col = chunks[c]
        some = my_rows
        if piece is not None:
            some = pl.ds(pl.multiple_of(me * rows + piece * piece_rows, piece_rows), piece_rows)
        block = readies[which].at[some, pl.ds(col * LANES, LANES)]
        return pltpu.make_async_remote_copy(
            src_ref=block,
            dst_ref=block,
            send_sem=out_send.at[k, c],
            recv_sem=out_recv.at[k, c],
            device_id={"shard": others[k]},
            device_id_type=MESH,
        )

    for c in range(len(chunks) + 1):
        if c < len(chunks):
            peak = jnp.zeros((SUBLANES, LANES), jnp.float32)
            if c == last:
                for piece in range(PIECES):
                    for read in reads(c, piece):
                        read.wait()
                    peak = update(c, piece * piece_rows, piece_rows, peak)
            else:
                for read in reads(c):
                    read.wait()
                if c + AHEAD <= last:
                    start_reads(c + AHEAD)
                peak = update(c, 0, rows, peak)
            peaks[c] = peak
            for k in range(peers - 1):
                peak_copy(c, k).start()
        if c >= 1:
            scale_and_round(c - 1)

    for c in range(len(chunks)):
        for k in range(peers - 1):
            peak_copy(c, k).wait_send()
            out_copy(c, k).wait_send()
            out_copy(c, k).wait_recv()


def store_kernel(pieces, *refs):
    half = len(refs) // 2
    sources, targets, sem = refs[:half], refs[half : 2 * half], refs[-1]
    copies = []
    for source, target in zip(sources, targets):
        parts = pieces if source.shape[0] % (pieces * LANES) == 0 else 1
        size = source.shape[0] // parts
        for p in range(parts):
            where = pl.ds(p * size, size)
            copies.append(
                pltpu.make_async_copy(source.at[where], target.at[where], sem.at[len(copies)])
            )
    for copy in copies:
        copy.start()
    for copy in copies:
        copy.wait()


def body(*arrays):
    *weights, norm_gain = arrays
    peers = lax.axis_size("shard")
    rows = norm_gain.shape[0]
    widths = [weights[3 * which].shape[1] for which in range(3)]
    chunks = [(which, col) for which in range(3) for col in range(widths[which] // LANES)]
    count = len(chunks)
    any_spec = pl.BlockSpec(memory_space=pltpu.HBM)
    vmem_spec = pl.BlockSpec(memory_space=pltpu.VMEM)
    ready_shapes = [((peers * rows, width), jnp.bfloat16) for width in widths]
    scale_shapes = [((width // LANES, LANES), jnp.float32) for width in widths]
    made = pl.pallas_call(
        functools.partial(exchange_kernel, peers, chunks),
        out_shape=[pltpu.VMEM(*s) for s in ready_shapes + scale_shapes],
        in_specs=[any_spec] * 10,
        out_specs=[vmem_spec] * 6,
        scratch_shapes=[
            pltpu.VMEM((rows // LANES, LANES), jnp.float32),
            pltpu.VMEM((3, count, rows, LANES), jnp.float32),
            pltpu.VMEM((rows, LANES), jnp.float32),
            pltpu.VMEM((count, SUBLANES, LANES), jnp.float32),
            pltpu.VMEM((peers - 1, count, SUBLANES, LANES), jnp.float32),
            pltpu.SemaphoreType.DMA,
            pltpu.SemaphoreType.DMA((3, count + PIECES - 1)),
            pltpu.SemaphoreType.DMA((peers - 1, count)),
            pltpu.SemaphoreType.DMA((peers - 1, count)),
            pltpu.SemaphoreType.DMA((peers - 1, count)),
            pltpu.SemaphoreType.DMA((peers - 1, count)),
        ],
        compiler_params=pltpu.CompilerParams(
            collective_id=0, has_side_effects=True, vmem_limit_bytes=44 * 1024 * 1024
        ),
        name="exchange",
    )(norm_gain.reshape(rows // LANES, LANES), *weights)
    pieces = 2
    stored = pl.pallas_call(
        functools.partial(store_kernel, pieces),
        out_shape=[jax.ShapeDtypeStruct(*s) for s in ready_shapes + scale_shapes],
        in_specs=[vmem_spec] * 6,
        out_specs=[any_spec] * 6,
        scratch_shapes=[pltpu.SemaphoreType.DMA((6 * pieces,))],
        compiler_params=pltpu.CompilerParams(vmem_limit_bytes=2 * 1024 * 1024),
        name="store",
    )(*made)
    return (*stored[:3], *(s.reshape(-1) for s in stored[3:]))


def solution(mesh):
    split = P(("shift", "shard"), "width")
    in_specs = (split,) * 9 + (P(("shift", "shard")),)
    out_specs = (P("shift", "width"),) * 3 + (P(("shift", "width")),) * 3
    return jax.shard_map(body, mesh=mesh, in_specs=in_specs, out_specs=out_specs, check_vma=False)
```
